8 devices in a mesh: rep: 2 (over y, z), dp: 4 (over x, core).
Axes of the slice: x: 2, y: 2, z: 1, core: 2. Of those that a mesh axis runs over, the one named last changes fastest.
Arguments:
- a: bfloat16 [8, 4, 4096, 768], P(('rep', 'dp')), parts along dimension 0
- g: bfloat16 [8, 4, 4096, 3072], P(('rep', 'dp')), parts along dimension 0
Outputs:
- output: bfloat16 [8, 768, 3072], P('rep'), parts along dimension 0
There are 2 independent parts. The reference program is written for one: setup_inputs(seed, part) draws one part's arguments, and reference() takes and returns one part's arrays. A program takes and returns all parts, laid end to end along the dimension named above; each array names one.
All inputs are finite; a program needn't handle non-finite values.
Results may differ from the reference program's by a relative error of at most 0.012.
Values are sent between devices in bfloat16 or wider.
A program may use at most 2 GiB of HBM per device.

```python
import jax
import jax.numpy as jnp
from jax import lax

DEVICES = 4
MATRICES = 4
TOKENS = 4096
D = 768
FF = 3072


def setup_inputs(seed: int = 0, part: int = 0) -> dict:
    ka, kg, ks = (jax.random.fold_in(k, part) for k in jax.random.split(jax.random.key(seed), 3))
    size = 2.0 ** jax.random.uniform(ks, (DEVICES, MATRICES, 1, 1), jnp.float32, -1.0, 1.0)
    a = jax.random.normal(ka, (DEVICES, MATRICES, TOKENS, D), jnp.float32)
    g = size * jax.random.normal(kg, (DEVICES, MATRICES, TOKENS, FF), jnp.float32) * (DEVICES * TOKENS) ** -0.5
    return {"a": a.astype(jnp.bfloat16), "g": g.astype(jnp.bfloat16)}


def reference(a, g):
    def take(so_far, one):
        return so_far + jnp.einsum("ntd,ntf->ndf", *one, preferred_element_type=jnp.float32), None

    return lax.scan(take, jnp.zeros((MATRICES, D, FF), jnp.float32), (a, g))[0].astype(jnp.bfloat16)
```

```python
import functools

import jax
import jax.numpy as jnp
from jax import lax
from jax.experimental import pallas as pl
from jax.experimental.pallas import tpu as pltpu
from jax.sharding import PartitionSpec as P

MESH = pl.DeviceIdType.MESH
WIDTH = 256
G_SLOTS = 3


def kernel(a_hbm, g_hbm, out, a_buf, a_t, g_buf, own, stage, came,
           a_sem, g_sem, d_send, d_recv, x_send, x_recv, f_send, f_recv):
    mats, tokens, rows = a_hbm.shape
    cols = g_hbm.shape[2]
    half = rows // 2
    tiles = cols // WIDTH
    steps = mats * tiles

    rep = lax.axis_index("rep")
    me = lax.axis_index("dp")
    core = lax.rem(me, 2)
    partner = me + 1 - 2 * core
    across = lax.rem(me + 2, 4)
    mine = pl.ds(pl.multiple_of(core * half, half), half)
    theirs = pl.ds(pl.multiple_of((1 - core) * half, half), half)

    def a_copy(n):
        return pltpu.make_async_copy(a_hbm.at[n], a_buf, a_sem)

    def g_copy(n, t, slot):
        return pltpu.make_async_copy(
            g_hbm.at[n, :, pl.ds(pl.multiple_of(t * WIDTH, WIDTH), WIDTH)],
            g_buf.at[slot], g_sem.at[slot])

    def block(n, t):
        return out.at[n, mine, pl.ds(pl.multiple_of(t * WIDTH, WIDTH), WIDTH)]

    def block_theirs(n, t):
        return out.at[n, theirs, pl.ds(pl.multiple_of(t * WIDTH, WIDTH), WIDTH)]

    def d_copy(n, t, i):
        return pltpu.make_async_remote_copy(
            stage.at[lax.rem(i, 2)], block_theirs(n, t), d_send.at[lax.rem(i, 2)], d_recv.at[i],
            device_id=(rep, partner), device_id_type=MESH)

    def d_arrival(n, t, i):
        return pltpu.make_async_remote_copy(
            stage.at[lax.rem(i, 2)], block(n, t), d_send.at[lax.rem(i, 2)], d_recv.at[i],
            device_id=(rep, partner), device_id_type=MESH)

    def x_copy(n, t, i):
        return pltpu.make_async_remote_copy(
            block(n, t), came.at[i], x_send.at[i], x_recv.at[i],
            device_id=(rep, across), device_id_type=MESH)

    def f_copy(n, t, i):
        return pltpu.make_async_remote_copy(
            block(n, t), block(n, t), f_send.at[i], f_recv.at[i],
            device_id=(rep, partner), device_id_type=MESH)

    def f_arrival(n, t, i):
        return pltpu.make_async_remote_copy(
            block_theirs(n, t), block_theirs(n, t), f_send.at[i], f_recv.at[i],
            device_id=(rep, partner), device_id_type=MESH)

    a_copy(0).start()
    for s in range(G_SLOTS - 1):
        g_copy(0, s, s).start()

    barrier = pltpu.get_barrier_semaphore()
    for other in (partner, across):
        pl.semaphore_signal(barrier, 1, device_id=(rep, other), device_id_type=MESH)
    pl.semaphore_wait(barrier, 2)

    @pl.loop(0, mats)
    def _(n):
        a_copy(n).wait()

        @pl.loop(0, tokens // 256)
        def _(k):
            at = pl.ds(pl.multiple_of(k * 256, 256), 256)
            a_t[:, at] = a_buf[at, :].T

        @pl.when(n + 1 < mats)
        def _():
            a_copy(n + 1).start()

        @pl.loop(0, tiles)
        def _(t):
            i = n * tiles + t
            slot = lax.rem(i, G_SLOTS)
            ahead = i + G_SLOTS - 1

            @pl.when(ahead < steps)
            def _():
                g_copy(ahead // tiles, lax.rem(ahead, tiles), lax.rem(ahead, G_SLOTS)).start()

            g_copy(n, t, slot).wait()

            @pl.when(i >= 2)
            def _():
                before = i - 2
                d_copy(before // tiles, lax.rem(before, tiles), before).wait_send()

            stage[lax.rem(i, 2)] = jnp.dot(
                a_t[theirs, :], g_buf[slot], preferred_element_type=jnp.float32
            ).astype(jnp.bfloat16)
            d_copy(n, t, i).start()
            own[...] = jnp.dot(a_t[mine, :], g_buf[slot], preferred_element_type=jnp.float32)
            d_arrival(n, t, i).wait_recv()
            b = block(n, t)
            b[...] = (own[...] + b[...].astype(jnp.float32)).astype(jnp.bfloat16)
            x_copy(n, t, i).start()

    for i in (steps - 2, steps - 1):
        d_copy(i // tiles, i % tiles, i).wait_send()

    @pl.loop(0, steps)
    def _(i):
        n, t = i // tiles, lax.rem(i, tiles)
        c = x_copy(n, t, i)
        c.wait_send()
        c.wait_recv()
        b = block(n, t)
        b[...] = (b[...].astype(jnp.float32) + came[i].astype(jnp.float32)).astype(jnp.bfloat16)
        f_copy(n, t, i).start()

    @pl.loop(0, steps)
    def _(i):
        n, t = i // tiles, lax.rem(i, tiles)
        f_copy(n, t, i).wait_send()
        f_arrival(n, t, i).wait_recv()


def solution(mesh):
    def step(a, g):
        a, g = a[0], g[0]
        mats, tokens, rows = a.shape
        cols = g.shape[2]
        half = rows // 2
        steps = mats * (cols // WIDTH)
        dma = pltpu.SemaphoreType.DMA
        return pl.pallas_call(
            kernel,
            out_shape=pltpu.VMEM((mats, rows, cols), jnp.bfloat16),
            in_specs=[pl.BlockSpec(memory_space=pl.ANY)] * 2,
            out_specs=pl.BlockSpec(memory_space=pltpu.VMEM),
            scratch_shapes=[
                pltpu.VMEM((tokens, rows), jnp.bfloat16),
                pltpu.VMEM((rows, tokens), jnp.bfloat16),
                pltpu.VMEM((G_SLOTS, tokens, WIDTH), jnp.bfloat16),
                pltpu.VMEM((half, WIDTH), jnp.float32),
                pltpu.VMEM((2, half, WIDTH), jnp.bfloat16),
                pltpu.VMEM((steps, half, WIDTH), jnp.bfloat16),
                dma, dma((G_SLOTS,)), dma((2,)), dma((steps,)),
                dma((steps,)), dma((steps,)), dma((steps,)), dma((steps,)),
            ],
            compiler_params=pltpu.CompilerParams(
                collective_id=0, has_side_effects=True, vmem_limit_bytes=42 << 20),
            name="sums",
        )(a, g)

    return jax.shard_map(
        step, mesh=mesh, in_specs=(P(("rep", "dp")), P(("rep", "dp"))), out_specs=P("rep"),
        check_vma=False)
```

```python
import jax
import jax.numpy as jnp
from jax import lax
from jax.experimental import pallas as pl
from jax.experimental.pallas import tpu as pltpu
from jax.sharding import PartitionSpec as P

MESH = pl.DeviceIdType.MESH
WIDTH = 512
PART = 128
FIRST = ((0, 128), (128, 256))


def kernel(a_hbm, g_hbm, out, a_buf, g_buf, own, stage, first_stage, came,
           a_first, a_sem, g_sem, d_send, first_send, d_recv,
           x_send, x_recv, f_send, f_recv):
    mats, tokens, rows = a_hbm.shape
    cols = g_hbm.shape[2]
    half = rows // 2
    tiles = cols // WIDTH
    steps = mats * tiles
    parts = half // PART
    f32, bf16 = jnp.float32, jnp.bfloat16

    rep = lax.axis_index("rep")
    me = lax.axis_index("dp")
    core = lax.rem(me, 2)
    partner = me + 1 - 2 * core
    across = lax.rem(me + 2, 4)

    def span(start, size, unit):
        return pl.ds(pl.multiple_of(start, unit), size)

    def block(which, n, r0, nr, c0, nc):
        return out.at[n, span(which * half + r0, nr, 64), span(c0, nc, 256)]

    def remote(src, dst, send, recv, to):
        return pltpu.make_async_remote_copy(
            src, dst, send, recv, device_id=(rep, to), device_id_type=MESH)

    def d_copy(src, send, recv, *at):
        return remote(src, block(1 - core, *at), send, recv, partner)

    def d_arrival(src, send, recv, *at):
        return remote(src, block(core, *at), send, recv, partner)

    def x_copy(j, n, r0, nr, c0, nc):
        return remote(block(core, n, r0, nr, c0, nc),
                      came.at[n, span(r0, nr, 64), span(c0, nc, 256)],
                      x_send.at[j], x_recv.at[j], across)

    def f_copy(j, *at):
        return remote(block(core, *at), block(core, *at), f_send.at[j], f_recv.at[j], partner)

    def f_arrival(j, *at):
        return remote(block(1 - core, *at), block(1 - core, *at), f_send.at[j], f_recv.at[j], partner)

    def a_copy(n):
        return pltpu.make_async_copy(a_hbm.at[n], a_buf.at[lax.rem(n, 2)], a_sem.at[lax.rem(n, 2)])

    def g_copy(i):
        return pltpu.make_async_copy(
            g_hbm.at[i // tiles, :, span(lax.rem(i, tiles) * WIDTH, WIDTH, WIDTH)],
            g_buf.at[lax.rem(i, 2)], g_sem.at[lax.rem(i, 2)])

    def term(which, slot, g, r0, nr):
        return lax.dot_general(
            a_buf[slot, :, span(which * half + r0, nr, 128)], g,
            (((0,), (0,)), ((), ())), preferred_element_type=f32)

    def add_term(b, value):
        b[...] = (value + b[...].astype(f32)).astype(bf16)

    def first_a(which, k):
        r0, nr = FIRST[k]
        at = span(which * half + r0, nr, 128)
        return pltpu.make_async_copy(
            a_hbm.at[0, :, at], a_buf.at[0, :, at], a_first.at[k, which])

    first_a(0, 0).start()
    first_a(1, 0).start()
    g_copy(0).start()
    first_a(0, 1).start()
    first_a(1, 1).start()
    g_copy(1).start()
    a_copy(1).start()

    barrier = pltpu.get_barrier_semaphore()
    for other in (partner, across):
        pl.semaphore_signal(barrier, 1, device_id=(rep, other), device_id_type=MESH)

    for k, (r0, nr) in enumerate(FIRST):
        first_a(0, k).wait()
        first_a(1, k).wait()
        if k == 0:
            g_copy(0).wait()
        at = (0, r0, nr, 0, WIDTH)
        g = g_buf.at[0]
        held = first_stage.at[k, pl.ds(0, nr)]
        held[...] = term(1 - core, 0, g[...], r0, nr).astype(bf16)
        if k == 0:
            pl.semaphore_wait(barrier, 2)
        d_copy(held, first_send.at[k], d_recv.at[k], *at).start()
        own[pl.ds(0, nr)] = term(core, 0, g[...], r0, nr)
        d_arrival(held, first_send.at[k], d_recv.at[k], *at).wait_recv()
        add_term(block(core, *at), own[pl.ds(0, nr)])
        x_copy(k, *at).start()

    def place(i):
        return i // tiles, lax.rem(i, tiles) * WIDTH

    def number(i, r):
        return len(FIRST) + (i - 1) * parts + r

    def tile_d(i):
        n, c0 = place(i)
        slot = lax.rem(i, 2)
        return stage.at[slot], d_send.at[slot], d_recv.at[len(FIRST) - 1 + i], n, 0, half, c0, WIDTH

    @pl.loop(1, steps)
    def _(i):
        n, c0 = place(i)
        slot = lax.rem(i, 2)

        @pl.when(i + 1 < steps)
        def _():
            g_copy(i + 1).start()

        @pl.when(c0 == 0)
        def _():
            a_copy(n).wait()

        @pl.when((c0 == 0) & (n + 1 < mats))
        def _():
            a_copy(n + 1).start()

        g_copy(i).wait()

        @pl.when(i >= 3)
        def _():
            d_copy(*tile_d(i - 2)).wait_send()

        stage[slot] = term(1 - core, lax.rem(n, 2), g_buf[slot], 0, half).astype(bf16)
        d_copy(*tile_d(i)).start()
        own[...] = term(core, lax.rem(n, 2), g_buf[slot], 0, half)
        d_arrival(*tile_d(i)).wait_recv()
        for r in range(parts):
            at = (n, r * PART, PART, c0, WIDTH)
            add_term(block(core, *at), own[pl.ds(r * PART, PART)])
            x_copy(number(i, r), *at).start()

    for k, (r0, nr) in enumerate(FIRST):
        d_copy(first_stage.at[k, pl.ds(0, nr)], first_send.at[k], d_recv.at[k],
               0, r0, nr, 0, WIDTH).wait_send()
    for i in (steps - 2, steps - 1):
        d_copy(*tile_d(i)).wait_send()

    def finish(j, n, r0, nr, c0, nc):
        at = (n, r0, nr, c0, nc)
        x_copy(j, *at).wait()
        add_term(block(core, *at), came[n, span(r0, nr, 64), span(c0, nc, 256)].astype(f32))
        f_copy(j, *at).start()

    for k, at in enumerate(FIRST):
        finish(k, 0, *at, 0, WIDTH)

    @pl.loop(1, steps)
    def _(i):
        n, c0 = place(i)
        for r in range(parts):
            finish(number(i, r), n, r * PART, PART, c0, WIDTH)

    for k, at in enumerate(FIRST):
        f_copy(k, 0, *at, 0, WIDTH).wait_send()
        f_arrival(k, 0, *at, 0, WIDTH).wait_recv()

    @pl.loop(1, steps)
    def _(i):
        n, c0 = place(i)
        for r in range(parts):
            at = (n, r * PART, PART, c0, WIDTH)
            f_copy(number(i, r), *at).wait_send()
            f_arrival(number(i, r), *at).wait_recv()


def solution(mesh):
    def step(a, g):
        a, g = a[0], g[0]
        mats, tokens, rows = a.shape
        cols = g.shape[2]
        half = rows // 2
        steps = mats * (cols // WIDTH)
        copies = len(FIRST) + (steps - 1) * (half // PART)
        dma = pltpu.SemaphoreType.DMA
        return pl.pallas_call(
            kernel,
            out_shape=pltpu.VMEM((mats, rows, cols), jnp.bfloat16),
            in_specs=[pl.BlockSpec(memory_space=pl.ANY)] * 2,
            out_specs=pl.BlockSpec(memory_space=pltpu.VMEM),
            scratch_shapes=[
                pltpu.VMEM((2, tokens, rows), jnp.bfloat16),
                pltpu.VMEM((2, tokens, WIDTH), jnp.bfloat16),
                pltpu.VMEM((half, WIDTH), jnp.float32),
                pltpu.VMEM((2, half, WIDTH), jnp.bfloat16),
                pltpu.VMEM((len(FIRST), half, WIDTH), jnp.bfloat16),
                pltpu.VMEM((mats, half, cols), jnp.bfloat16),
                dma((2, 2)), dma((2,)), dma((2,)), dma((2,)), dma((len(FIRST),)),
                dma((len(FIRST) + steps - 1,)),
                dma((copies,)), dma((copies,)), dma((copies,)), dma((copies,)),
            ],
            compiler_params=pltpu.CompilerParams(
                collective_id=0, has_side_effects=True, vmem_limit_bytes=42 << 20),
            name="sums",
        )(a, g)

    return jax.shard_map(
        step, mesh=mesh, in_specs=(P(("rep", "dp")), P(("rep", "dp"))), out_specs=P("rep"),
        check_vma=False)
```
